32 devices in a mesh: clump: 8 (over z, y), grp: 4 (over x, core).
Axes of the slice: x: 2, y: 2, z: 4, core: 2. Of those that a mesh axis runs over, the one named last changes fastest.
Arguments:
- flux: float32 [32, 1024, 64], P(('clump', 'grp')), may hold values from -6 to 6
- patch_pft: int32 [32, 1024], P(('clump', 'grp')), may hold values from 0 to 15
- patch_wt: float32 [32, 1024], P(('clump', 'grp')), may hold values from 0.2 to 2
- patch_col: int32 [32, 1024], P(('clump', 'grp')), may hold values from 0 to 511, never falling along the last dimension, each value on 1 to 4 neighbouring positions
- col_wt: float32 [32, 512], P(('clump', 'grp')), may hold values from 0.2 to 2
- col_lu: int32 [32, 512], P(('clump', 'grp')), may hold values from 0 to 255, never falling along the last dimension, each value on 1 to 4 neighbouring positions
- lu_wt: float32 [32, 256], P(('clump', 'grp')), may hold values from 0.2 to 2
- lu_grid: int32 [32, 256], P(('clump', 'grp')), may hold values from 0 to 127, never falling along the last dimension, each value on 1 to 4 neighbouring positions
- cell_target: int32 [32, 128], P(('clump', 'grp')), may hold values from 0 to 4095, as said below
- patch_count: int32 [32], P(('clump', 'grp')), may hold values from 64 to 1024
- pft_scale: float32 [16, 64], replicated, may hold values from 0.3 to 3
- cpl_frac: float32 [4096], P(('clump', 'grp')), may hold values from 0.2 to 0.9
- cpl_field: float32 [4096, 64], P(('clump', 'grp')), may hold values from -6 to 6
Outputs:
- grid_merged: float32 [4096, 64], P(('clump', 'grp'))
- anomaly: float32 [32, 1024, 64], P(('clump', 'grp'))
The draws below stay inside these ranges and needn't reach their ends.
Inputs may be any that keep to these rules, and one draw needn't show every extreme that they name: `patch_col`: within each device's row the column numbers never fall, and each column holds 1 to 4 patch slots. `col_lu`: within each device's row the landunit numbers never fall, and each landunit holds 1 to 4 columns. `lu_grid`: within each device's row the gridcell numbers never fall, and each gridcell holds 1 to 4 landunits. `cell_target`: all devices' entries together are a permutation of 0 to 4095; the coupler owner of an entry q is q // 128, and each device's 128 gridcells go to 16 owners, exactly 8 to each.
All inputs are finite; a program needn't handle non-finite values.
Results may differ from the reference program's by a relative error of at most 0.0003.
Values sent between devices are 32-bit elements; how exact they have to be, the bound alone decides.
A program may use at most 64 MiB of HBM per device.

```python
import math
import jax
import jax.numpy as jnp
import numpy as np
from jax import lax

NV = 64
NPFT = 16
P_DEV = 1024
C_DEV = 512
L_DEV = 256
G_DEV = 128
CAP = 8
GRID = 4096
DEVICES = 32


def row_orders(key, rows, length):

    def single(row_key):
        return jax.random.permutation(row_key, length)
    return jax.vmap(single)(jax.random.split(key, rows))


def draw_cell_target(key, part):
    key_shift, key_label, key_local, key_slot = jax.random.split(jax.random.fold_in(key, 11), 4)
    shift = jax.random.permutation(key_shift, DEVICES).astype(jnp.int32)
    label = jax.random.permutation(key_label, DEVICES).astype(jnp.int32)
    local_order = row_orders(key_local, DEVICES, G_DEV).astype(jnp.int32)
    slot_order = row_orders(key_slot, DEVICES, G_DEV).astype(jnp.int32)
    block_of = local_order // CAP
    pre_owner = (block_of + shift[:, None]) % DEVICES
    owner_dev = label[pre_owner]
    slot_in = slot_order[pre_owner, local_order]
    return (owner_dev * G_DEV + slot_in).astype(jnp.int32)


def place_ends(result, key, least, largest):
    index_at = [jax.random.randint(jax.random.fold_in(key, axis), (), 0, length) for axis, length in enumerate(result.shape)]
    widest = result.shape.index(max(result.shape))
    beside = index_at[:widest] + [(index_at[widest] + 1) % result.shape[widest]] + index_at[widest + 1:]
    return result.at[tuple(index_at)].set(least).at[tuple(beside)].set(largest)


def steps_of(key, dims, cuts, smallest, high):
    factor_of = 1.0
    for dim, parts in cuts:
        steps = jax.random.uniform(jax.random.fold_in(jax.random.fold_in(key, 6), dim), (parts,), jnp.float32, smallest / len(cuts), high / len(cuts))
        factor_of = factor_of * jnp.repeat(jnp.exp(steps), dims[dim] // parts).reshape((-1,) + (1,) * (len(dims) - 1 - dim))
    return factor_of


def split_up(count, total, most, lean):
    loads = [(1 << 20) // math.isqrt(standing ** lean) + 1 for standing in range(2, count + 1)]
    spare, counts = total - most - (count - 1), [1] * (count - 1)
    while spare > 0:
        candidates = [i for i in range(count - 1) if counts[i] < most]
        mass, left = sum([loads[i] for i in candidates]), spare
        for i in candidates:
            more = min(most - counts[i], max(1, left * loads[i] // mass), spare)
            counts[i] = counts[i] + more
            spare = spare - more
    return np.array([most] + counts)


def ragged(own_key, number_of, total, most, slope):
    if number_of == 2:
        one = jax.random.randint(own_key, (), max(1, total - most), min(most, total - 1) + 1)
        return jnp.stack([one, total - one])
    tallies = jnp.asarray(split_up(number_of, total, most, slope), jnp.int32)
    couples = (number_of - 1) // 2
    giver, sink = tallies[1:1 + 2 * couples:2], tallies[2:2 + 2 * couples:2]
    margin = jnp.minimum(giver - 1, most - sink)
    passed = jax.random.randint(jax.random.fold_in(own_key, 1), (couples,), 0, 1 << 20) % (margin + 1)
    tallies = tallies.at[1:1 + 2 * couples:2].set(giver - passed).at[2:2 + 2 * couples:2].set(sink + passed)
    return tallies[jax.random.permutation(jax.random.fold_in(own_key, 2), number_of)]


def gaussian(rng, dims, deviation, reach, pieces=(), kind=jnp.bfloat16):
    factor_of = steps_of(rng, dims, pieces, -0.22, 0.18) if pieces else 1.0
    array = jax.random.normal(rng, dims, jnp.float32) * deviation * factor_of
    return jnp.minimum(jnp.maximum(array, -reach), reach).astype(kind)


def setup_inputs(seed: int = 0) -> dict:
    seeds = jax.random.split(jax.random.key(seed), 14)
    flux = gaussian(seeds[0], (DEVICES, P_DEV, NV), 1.0, 6.0, ((0, 32),), jnp.float32)
    patch_pft = place_ends(jax.random.randint(seeds[1], (DEVICES, P_DEV), 0, NPFT), jax.random.fold_in(seeds[1], 1), 0, NPFT - 1).astype(jnp.int32)
    patch_wt = jnp.clip(jnp.exp(math.log(2.0) - 2.3025851 * jax.random.uniform(seeds[2], (DEVICES, P_DEV), jnp.float32) ** steps_of(seeds[2], (DEVICES, P_DEV), ((0, 32),), -0.2, 0.2)), 0.2, 2.0)
    patch_col = jax.vmap(lambda own: jnp.searchsorted(jnp.cumsum(ragged(own, C_DEV, P_DEV, 4, 1)), jnp.arange(P_DEV), side="right"))(jax.random.split(seeds[3], DEVICES)).reshape((DEVICES, P_DEV)).astype(jnp.int32)
    col_wt = jnp.clip(jnp.exp(math.log(2.0) - 2.3025851 * jax.random.uniform(seeds[4], (DEVICES, C_DEV), jnp.float32) ** steps_of(seeds[4], (DEVICES, C_DEV), ((0, 32),), -0.2, 0.2)), 0.2, 2.0)
    col_lu = jax.vmap(lambda own: jnp.searchsorted(jnp.cumsum(ragged(own, L_DEV, C_DEV, 4, 1)), jnp.arange(C_DEV), side="right"))(jax.random.split(seeds[5], DEVICES)).reshape((DEVICES, C_DEV)).astype(jnp.int32)
    lu_wt = jnp.clip(jnp.exp(math.log(2.0) - 2.3025851 * jax.random.uniform(seeds[6], (DEVICES, L_DEV), jnp.float32) ** steps_of(seeds[6], (DEVICES, L_DEV), ((0, 32),), -0.2, 0.2)), 0.2, 2.0)
    lu_grid = jax.vmap(lambda own: jnp.searchsorted(jnp.cumsum(ragged(own, G_DEV, L_DEV, 4, 1)), jnp.arange(L_DEV), side="right"))(jax.random.split(seeds[7], DEVICES)).reshape((DEVICES, L_DEV)).astype(jnp.int32)
    cell_target = draw_cell_target(jax.random.fold_in(seeds[13], 71), 0)
    patch_count = place_ends(jax.random.randint(seeds[9], (DEVICES,), P_DEV // 16, P_DEV + 1), jax.random.fold_in(seeds[9], 1), P_DEV // 16, P_DEV).astype(jnp.int32)
    pft_scale = jnp.clip(jnp.exp(jax.random.uniform(seeds[10], (NPFT, NV), jnp.float32, math.log(0.3), math.log(3.0))), 0.3, 3.0)
    cpl_frac = jnp.clip(0.2 + 0.7 * jax.random.uniform(seeds[11], (GRID,), jnp.float32) ** steps_of(seeds[11], (GRID,), ((0, 32),), -0.2, 0.2), 0.2, 0.9)
    cpl_field = gaussian(seeds[12], (GRID, NV), 1.0, 6.0, ((0, 32),), jnp.float32)
    return {"flux": flux, "patch_pft": patch_pft, "patch_wt": patch_wt, "patch_col": patch_col, "col_wt": col_wt, "col_lu": col_lu, "lu_wt": lu_wt, "lu_grid": lu_grid, "cell_target": cell_target, "patch_count": patch_count, "pft_scale": pft_scale, "cpl_frac": cpl_frac, "cpl_field": cpl_field}


def reference(flux, patch_pft, patch_wt, patch_col, col_wt, col_lu, lu_wt, lu_grid, cell_target, patch_count, pft_scale, cpl_frac, cpl_field):
    position = jnp.arange(P_DEV, dtype=jnp.int32)

    def local_means(entries):
        values, pft_ids, pweight, columns, cweight, colland, lweight, lugrid, live_count = entries
        alive_mask = (position < live_count).astype(jnp.float32)
        scaled = values * pft_scale[pft_ids]
        land_of = colland[columns]
        home_of = lugrid[land_of]
        weight_eff = alive_mask * pweight * cweight[columns] * lweight[land_of]
        numer = jax.ops.segment_sum(scaled * weight_eff[:, None], home_of, G_DEV)
        denom = jax.ops.segment_sum(weight_eff, home_of, G_DEV)
        return numer / jnp.maximum(denom, 1.0)[:, None]

    cell_mean = lax.map(local_means, (flux, patch_pft, patch_wt, patch_col, col_wt, col_lu, lu_wt, lu_grid, patch_count))
    placed = jnp.zeros((GRID, NV), jnp.float32).at[cell_target.reshape(-1)].set(cell_mean.reshape(-1, NV))
    grid_merged = cpl_frac[:, None] * placed + (1.0 - cpl_frac)[:, None] * cpl_field

    def local_anomaly(entries):
        values, pft_ids, columns, colland, lugrid, targets, live_count = entries
        alive_mask = (position < live_count).astype(jnp.float32)
        scaled = values * pft_scale[pft_ids]
        home_of = lugrid[colland[columns]]
        cell_merged = grid_merged[targets]
        return alive_mask[:, None] * (scaled - cell_merged[home_of])

    anomaly = lax.map(local_anomaly, (flux, patch_pft, patch_col, col_lu, lu_grid, cell_target, patch_count))
    return grid_merged, anomaly
```

```python
import functools

import jax
import jax.numpy as jnp
from jax import lax
from jax.experimental import pallas as pl
from jax.experimental.pallas import tpu as pltpu
from jax.sharding import PartitionSpec as P

MESH = pl.DeviceIdType.MESH
F32 = jnp.float32
BF16 = jnp.bfloat16


def iota(shape, dim):
    return lax.broadcasted_iota(jnp.int32, shape, dim)


def onehot(mask):
    return jnp.where(mask, 1.0, 0.0).astype(BF16)


def halves(x):
    high = x.astype(BF16)
    return high, (x - high.astype(F32)).astype(BF16)


def dot(a, b):
    return jnp.dot(a, b, preferred_element_type=F32)


def dot_nt(a, b):
    return lax.dot_general(a, b, (((1,), (1,)), ((), ())), preferred_element_type=F32)


def rows_of(rows, total):
    n = rows[0].shape[1]
    at = iota((total, n), 0)
    out = jnp.zeros((total, n), F32)
    for k, row in enumerate(rows):
        out = jnp.where(at == k, jnp.broadcast_to(row.astype(F32), (total, n)), out)
    return out.astype(BF16)


def kernel(
    n_clump, n_group, cap,
    count_ref, flux_ref, pft_ref, pwt_ref, pcol_ref, cwt_ref, clu_ref, lwt_ref, lgrid_ref,
    target_ref, scale_ref, frac_ref, field_ref,
    merged_ref, anomaly_ref,
    send, recv, reply, back, send_sem, recv_sem,
):
    n = n_clump * n_group
    me = lax.axis_index("clump") * n_group + lax.axis_index("grp")

    def device(index):
        return (index // n_group, index % n_group)

    barrier = pltpu.get_barrier_semaphore()

    def greet(j, carry):
        pl.semaphore_signal(
            barrier, inc=1, device_id=device((me + j) % n), device_id_type=MESH
        )
        return carry

    lax.fori_loop(1, n, greet, 0)

    nv, patches = flux_ref.shape
    types = scale_ref.shape[0]
    cols = cwt_ref.shape[1]
    lus = lwt_ref.shape[1]
    cells = target_ref.shape[1]
    slots = n * cap

    lu_hi, lu_lo = halves(lwt_ref[...])
    lu_rows = rows_of([lu_hi, lu_lo, lgrid_ref[...]], 16)
    lu_of = onehot(iota((lus, cols), 0) == clu_ref[...])
    col_vals = dot(lu_rows, lu_of)
    col_w = cwt_ref[...] * (col_vals[0:1] + col_vals[1:2])
    c_hi, c_lo = halves(col_w)
    col_rows = rows_of([c_hi, c_lo, col_vals[2:3]], 16)
    col_of = onehot(iota((cols, patches), 0) == pcol_ref[...])
    patch_vals = dot(col_rows, col_of)
    alive = jnp.where(iota((1, patches), 1) < count_ref[0], 1.0, 0.0)
    weight = alive * pwt_ref[...] * (patch_vals[0:1] + patch_vals[1:2])
    home = patch_vals[2:3].astype(jnp.int32)
    home_of = onehot(iota((cells, patches), 0) == home)

    table = scale_ref[...]
    t1 = table.astype(BF16).astype(F32)
    t2 = (table - t1).astype(BF16).astype(F32)
    t3 = table - t1 - t2
    pad = 128 - 3 * types
    stacked = jnp.concatenate([t1, t2, t3, jnp.zeros((pad, nv), F32)], axis=0)
    stacked = jnp.concatenate([stacked, jnp.zeros((128, 128 - nv), F32)], axis=1)
    scale_t = stacked.T[:nv].astype(BF16)
    kind = iota((128, patches), 0)
    type_of = onehot(
        (kind == pft_ref[...])
        | (kind == pft_ref[...] + types)
        | (kind == pft_ref[...] + 2 * types)
    )
    scaled = flux_ref[...] * dot(scale_t, type_of)

    x_hi, x_lo = halves(scaled * weight)
    w_hi, w_lo = halves(weight)
    sums = dot_nt(
        jnp.concatenate([x_hi, x_lo, rows_of([w_hi, w_lo], 16)], axis=0), home_of
    )
    num = sums[:nv] + sums[nv : 2 * nv]
    den = sums[2 * nv : 2 * nv + 1] + sums[2 * nv + 1 : 2 * nv + 2]
    mean = num / jnp.maximum(den, 1.0)

    target = target_ref[...]
    owner = target // cells
    local = target - owner * cells
    owner_b = jnp.broadcast_to(owner.astype(F32), (cells, cells))
    same = owner_b == owner_b.T
    earlier = iota((cells, cells), 0) < iota((cells, cells), 1)
    rank = jnp.sum(jnp.where(same & earlier, 1.0, 0.0), axis=0, keepdims=True).astype(jnp.int32)
    ahead = owner - me
    ahead = jnp.where(ahead < 0, ahead + n, ahead)
    slot = ahead * cap + rank
    slot_of = onehot(iota((slots, cells), 0) == slot)

    m_hi, m_lo = halves(mean)
    pad_rows = 128 - nv
    ids = rows_of([local + 1], pad_rows)
    left = jnp.concatenate([m_hi, ids], axis=0)
    right = jnp.concatenate([m_lo, jnp.zeros((pad_rows, cells), BF16)], axis=0)
    send[...] = dot_nt(slot_of, left) + dot_nt(slot_of, right)
    recv[0:cap, :] = send[0:cap, :]

    pl.semaphore_wait(barrier, n - 1)

    def copy(source, into, k, j, where):
        rows = pl.ds(pl.multiple_of(j * cap, cap), cap)
        return pltpu.make_async_remote_copy(
            src_ref=source.at[rows],
            dst_ref=into.at[rows],
            send_sem=send_sem.at[k],
            recv_sem=recv_sem.at[k],
            device_id=device(where),
            device_id_type=MESH,
        )

    def forth(j, carry):
        copy(send, recv, 0, j, (me + j) % n).start()
        return carry

    def home_again(j, carry):
        copy(reply, back, 1, j, (me + n - j) % n).start()
        return carry

    def wait(buffer, sem):
        rest = buffer.at[pl.ds(cap, slots - cap)]
        pltpu.make_async_copy(rest, rest, sem).wait()

    lax.fori_loop(1, n, forth, 0)
    wait(recv, recv_sem.at[0])

    got = recv[...]
    got_ids = got[:, nv : nv + 1].astype(jnp.int32)
    owned_of = onehot(iota((slots, cells), 1) + 1 == got_ids)
    g_hi, g_lo = halves(got.T[:nv])
    both = dot(jnp.concatenate([g_hi, g_lo], axis=0), owned_of)
    frac = frac_ref[...]
    merged = frac * (both[:nv] + both[nv:]) + (1.0 - frac) * field_ref[...]
    merged_ref[...] = merged
    r_hi, r_lo = halves(merged)
    blank = jnp.zeros((pad_rows, cells), BF16)
    reply[...] = dot_nt(owned_of, jnp.concatenate([r_hi, blank], axis=0)) + dot_nt(
        owned_of, jnp.concatenate([r_lo, blank], axis=0)
    )
    back[0:cap, :] = reply[0:cap, :]
    lax.fori_loop(1, n, home_again, 0)
    wait(back, recv_sem.at[1])

    b_hi, b_lo = halves(back[...].T[:nv])
    cell = dot(jnp.concatenate([b_hi, b_lo], axis=0), slot_of)
    c_hi, c_lo = halves(cell[:nv] + cell[nv:])
    picked = dot(jnp.concatenate([c_hi, c_lo], axis=0), home_of)
    anomaly_ref[...] = alive * (scaled - (picked[:nv] + picked[nv:]))
    wait(send, send_sem.at[0])
    wait(reply, send_sem.at[1])


def per_device(
    flux, patch_pft, patch_wt, patch_col, col_wt, col_lu, lu_wt, lu_grid, cell_target,
    patch_count, pft_scale, cpl_frac, cpl_field,
):
    n_clump = lax.axis_size("clump")
    n_group = lax.axis_size("grp")
    n = n_clump * n_group
    nv = flux.shape[2]
    patches = flux.shape[1]
    cells = cell_target.shape[1]
    cap = max(2, 2 * cells // n)
    cap = -(-cap // 8) * 8
    vmem = pl.BlockSpec(memory_space=pltpu.VMEM)
    buffer = pltpu.VMEM((n * cap, 128), F32)
    merged, anomaly = pl.pallas_call(
        functools.partial(kernel, n_clump, n_group, cap),
        out_shape=(
            jax.ShapeDtypeStruct((nv, cells), F32),
            jax.ShapeDtypeStruct((nv, patches), F32),
        ),
        in_specs=[pl.BlockSpec(memory_space=pltpu.SMEM)] + [vmem] * 12,
        out_specs=(vmem, vmem),
        scratch_shapes=[
            buffer, buffer, buffer, buffer,
            pltpu.SemaphoreType.DMA((2,)),
            pltpu.SemaphoreType.DMA((2,)),
        ],
        compiler_params=pltpu.CompilerParams(collective_id=0, has_side_effects=True),
    )(
        patch_count, flux[0].T, patch_pft, patch_wt, patch_col, col_wt, col_lu, lu_wt,
        lu_grid, cell_target, pft_scale, cpl_frac.reshape(1, -1), cpl_field.T,
    )
    return merged.T, anomaly.T[None]


def solution(mesh):
    split = P(("clump", "grp"))
    return jax.shard_map(
        per_device,
        mesh=mesh,
        in_specs=(split,) * 10 + (P(),) + (split,) * 2,
        out_specs=(split, split),
        check_vma=False,
    )
```

```python
import functools

import jax
import jax.numpy as jnp
from jax import lax
from jax.experimental import pallas as pl
from jax.experimental.pallas import tpu as pltpu
from jax.sharding import PartitionSpec as P

MESH = pl.DeviceIdType.MESH
F32 = jnp.float32
BF16 = jnp.bfloat16
INPUTS = 12


def iota(shape, dim):
    return lax.broadcasted_iota(jnp.int32, shape, dim)


def onehot(mask):
    return jnp.where(mask, 1.0, 0.0).astype(BF16)


def halves(x):
    high = x.astype(BF16)
    return high, (x - high.astype(F32)).astype(BF16)


def dot(a, b):
    return jnp.dot(a, b, preferred_element_type=F32)


def dot_nt(a, b):
    return lax.dot_general(a, b, (((1,), (1,)), ((), ())), preferred_element_type=F32)


def rows_of(rows, total):
    n = rows[0].shape[1]
    at = iota((total, n), 0)
    out = jnp.zeros((total, n), F32)
    for k, row in enumerate(rows):
        out = jnp.where(at == k, jnp.broadcast_to(row.astype(F32), (total, n)), out)
    return out.astype(BF16)


def split_by(x, size):
    if size & (size - 1) == 0:
        return lax.shift_right_logical(x, jnp.int32(size.bit_length() - 1)), x & (size - 1)
    return x // size, x % size


def select(table, chosen):
    high, low = halves(table)
    both = dot(jnp.concatenate([high, low], axis=0), chosen)
    return both[: table.shape[0]] + both[table.shape[0] :]


def pack(chosen, x):
    rows = chosen.shape[0] // 2
    pair = jnp.concatenate([chosen[:rows], chosen[rows:]], axis=1)
    blank = jnp.zeros(x.shape, BF16)

    def wide(part):
        upper = jnp.concatenate([part, blank], axis=1)
        return jnp.concatenate([upper, jnp.concatenate([blank, part], axis=1)], axis=0)

    high, low = halves(x)
    return dot_nt(pair, wide(high)) + dot_nt(pair, wide(low))


def unpack(packed):
    turned = packed.T
    middle = turned.shape[0] // 2
    return jnp.concatenate([turned[:middle], turned[middle:]], axis=1)


def kernel(
    n_clump, n_group, cap, half, stride,
    *refs,
):
    count_ref, *refs = refs
    sources, refs = refs[:INPUTS], refs[INPUTS:]
    merged_ref, anomaly_ref = refs[:2]
    send, recv, reply, back, ask, asked, send_sem, recv_sem, in_sem = refs[2:11]
    staged = refs[11:]
    loads = [
        pltpu.make_async_copy(source, into, in_sem.at[k])
        for k, (source, into) in enumerate(zip(sources, staged))
    ]
    (
        target_ref, lwt_ref, lgrid_ref, clu_ref, cwt_ref, pcol_ref, pwt_ref,
        scale_ref, pft_ref, flux_ref, frac_ref, field_ref,
    ) = staged
    n = n_clump * n_group
    my_clump, my_group = lax.axis_index("clump"), lax.axis_index("grp")

    def ahead_of(mine, step, size):
        there = mine + step
        return jnp.where(there >= size, there - size, there)

    def behind(mine, step, size):
        there = mine - step
        return jnp.where(there < 0, there + size, there)

    def each_other(act, there):
        groups = [there(my_group, g, n_group) for g in range(n_group)]

        def row(c, first):
            clump = there(my_clump, c, n_clump)
            for g in range(first, n_group):
                act(c * n_group + g, (clump, groups[g]))

        row(0, 1)
        if n_clump <= 8:
            for c in range(1, n_clump):
                row(c, 0)
        else:

            @pl.loop(1, n_clump)
            def _(c):
                row(c, 0)

    barrier = pltpu.get_barrier_semaphore()

    def greet(block, device):
        pl.semaphore_signal(barrier, inc=1, device_id=device, device_id_type=MESH)

    each_other(greet, ahead_of)
    for load in loads:
        load.start()

    nv, patches = flux_ref.shape
    types = scale_ref.shape[0]
    cols = cwt_ref.shape[1]
    lus = lwt_ref.shape[1]
    cells = target_ref.shape[1]
    rows = n * stride

    loads[0].wait()
    target = target_ref[...]
    owner, local = split_by(target, cells)
    owner_b = jnp.broadcast_to(owner.astype(F32), (cells, cells))
    same = owner_b == owner_b.T
    earlier = iota((cells, cells), 0) < iota((cells, cells), 1)
    rank = jnp.sum(jnp.where(same & earlier, 1.0, 0.0), axis=0, keepdims=True).astype(jnp.int32)
    to_clump, to_group = split_by(owner, n_group)
    block = behind(to_clump, my_clump, n_clump) * n_group
    block = (block + behind(to_group, my_group, n_group)) * stride
    from_block = behind(my_clump, to_clump, n_clump) * n_group
    from_block = (from_block + behind(my_group, to_group, n_group)) * stride
    part, line = split_by(rank, half)
    slot_of = onehot(iota((2 * rows, cells), 0) == part * rows + block + line)

    loads[10].wait()
    frac = frac_ref[...]
    at = iota((rows, cells), 0)
    asks = jnp.where(at == block, (local + 1).astype(F32), 0.0).astype(BF16)
    ask_rows = dot_nt(asks, onehot(iota((128, cells), 0) == rank))
    second = split_by(iota((rows, 128), 0), stride)[1] == 1
    ask[...] = jnp.where(second, jnp.broadcast_to(frac, (rows, cells)), ask_rows)
    asked[0:2, :] = ask[0:2, :]
    for load in loads[1:5]:
        load.wait()
    def copy(source, into, k, count, block, device):
        start = block * stride
        lines = pl.ds(start if isinstance(start, int) else pl.multiple_of(start, stride), count)
        return pltpu.make_async_remote_copy(
            src_ref=source.at[lines],
            dst_ref=into.at[lines],
            send_sem=send_sem.at[k],
            recv_sem=recv_sem.at[k],
            device_id=device,
            device_id_type=MESH,
        )

    def send_all(source, into, k, count, there):
        def one(block, device):
            copy(source, into, k, count, block, device).start()

        each_other(one, there)

    def wait(buffer, sem, count):
        rest = buffer.at[pl.ds(0, (n - 1) * count)]
        pltpu.make_async_copy(rest, rest, sem).wait()

    lu_hi, lu_lo = halves(lwt_ref[...])
    lu_rows = rows_of([lu_hi, lu_lo, lgrid_ref[...]], 16)
    lu_of = onehot(iota((lus, cols), 0) == clu_ref[...])
    col_vals = dot(lu_rows, lu_of)
    col_w = cwt_ref[...] * (col_vals[0:1] + col_vals[1:2])
    pl.semaphore_wait(barrier, n - 1)
    send_all(ask, asked, 0, 2, ahead_of)

    for load in loads[5:7]:
        load.wait()
    c_hi, c_lo = halves(col_w)
    col_rows = rows_of([c_hi, c_lo, col_vals[2:3]], 16)
    col_of = onehot(iota((cols, patches), 0) == pcol_ref[...])
    patch_vals = dot(col_rows, col_of)
    alive = jnp.where(iota((1, patches), 1) < count_ref[0], 1.0, 0.0)
    weight = alive * pwt_ref[...] * (patch_vals[0:1] + patch_vals[1:2])
    home = patch_vals[2:3].astype(jnp.int32)
    home_of = onehot(iota((cells, patches), 0) == home)

    for load in loads[7:10]:
        load.wait()
    table = scale_ref[...]
    t1 = table.astype(BF16).astype(F32)
    t2 = (table - t1).astype(BF16).astype(F32)
    t3 = table - t1 - t2
    pad = 128 - 3 * types
    stacked = jnp.concatenate([t1, t2, t3, jnp.zeros((pad, nv), F32)], axis=0)
    stacked = jnp.concatenate([stacked, jnp.zeros((128, 128 - nv), F32)], axis=1)
    scale_t = stacked.T[:nv].astype(BF16)
    kind = iota((128, patches), 0)
    type_of = onehot(
        (kind == pft_ref[...])
        | (kind == pft_ref[...] + types)
        | (kind == pft_ref[...] + 2 * types)
    )
    scaled = flux_ref[...] * dot(scale_t, type_of)

    x_hi, x_lo = halves(scaled * weight)
    w_hi, w_lo = halves(weight)
    sums = dot_nt(
        jnp.concatenate([x_hi, x_lo, rows_of([w_hi, w_lo], 16)], axis=0), home_of
    )
    num = sums[:nv] + sums[nv : 2 * nv]
    den = sums[2 * nv : 2 * nv + 1] + sums[2 * nv + 1 : 2 * nv + 2]
    mean = num / jnp.maximum(den, 1.0)

    send[...] = pack(slot_of, mean)
    recv[0:half, :] = send[0:half, :]
    send_all(send, recv, 1, half, ahead_of)

    loads[11].wait()
    other = (1.0 - frac) * field_ref[...]
    lane = iota((2 * rows, 128), 0)
    lane_part = jnp.where(lane >= rows, 1, 0)
    lane_line = split_by(lane - lane_part * rows, stride)[1]
    its_lane = (lane_line < half) & (
        iota((2 * rows, 128), 1) == lane_part * half + lane_line
    )
    in_two = split_by(iota((rows, 128), 0), stride)[1] < 2
    in_half = split_by(iota((rows, 128), 0), stride)[1] < half
    wait(asked, recv_sem.at[0], 2)
    told = jnp.where(in_two, asked[...], 0.0)
    ids_of = jnp.broadcast_to(
        told.reshape(n, stride, 128)[:, 0:1, :], (n, stride, 128)
    ).reshape(rows, 128)
    spread = jnp.where(its_lane, jnp.concatenate([ids_of, ids_of], axis=0), 0.0).astype(BF16)
    ids = dot(spread, jnp.ones((128, cells), BF16))
    owned_of = onehot(ids == (iota((2 * rows, cells), 1) + 1).astype(F32))
    reply[...] = pack(owned_of, other)
    back[0:half, :] = reply[0:half, :]
    send_all(reply, back, 2, half, behind)

    all_frac = select(told.T, onehot(iota((rows, cells), 0) == from_block + 1))
    cell_frac = jnp.sum(
        jnp.where(iota((128, cells), 0) == local, all_frac, 0.0), axis=0, keepdims=True
    )
    land_part = cell_frac * mean

    wait(recv, recv_sem.at[1], half)
    owned = select(unpack(jnp.where(in_half, recv[...], 0.0)), owned_of)
    merged_ref[...] = frac * owned + other

    wait(back, recv_sem.at[2], half)
    cell = land_part + select(unpack(jnp.where(in_half, back[...], 0.0)), slot_of)
    anomaly_ref[...] = alive * (scaled - select(cell, home_of))
    wait(ask, send_sem.at[0], 2)
    wait(send, send_sem.at[1], half)
    wait(reply, send_sem.at[2], half)


def store_kernel(merged, anomaly, merged_out, anomaly_out, sem):
    stores = [
        pltpu.make_async_copy(merged, merged_out, sem.at[0]),
        pltpu.make_async_copy(anomaly, anomaly_out, sem.at[1]),
    ]
    for store in stores:
        store.start()
    for store in stores:
        store.wait()


def per_device(
    flux, patch_pft, patch_wt, patch_col, col_wt, col_lu, lu_wt, lu_grid, cell_target,
    patch_count, pft_scale, cpl_frac, cpl_field,
):
    n_clump = lax.axis_size("clump")
    n_group = lax.axis_size("grp")
    n = n_clump * n_group
    nv = flux.shape[2]
    patches = flux.shape[1]
    cells = cell_target.shape[1]
    cap = max(2, 2 * cells // n)
    half = -(-cap // 2)
    stride = -(-max(half, 2) // 8) * 8
    vmem = pl.BlockSpec(memory_space=pltpu.VMEM)
    hbm = pl.BlockSpec(memory_space=pltpu.HBM)
    buffer = pltpu.VMEM((n * stride, 128), F32)
    inputs = (
        cell_target, lu_wt, lu_grid, col_lu, col_wt, patch_col, patch_wt,
        pft_scale, patch_pft, flux[0].T, cpl_frac.reshape(1, -1), cpl_field.T,
    )
    shapes = (
        jax.ShapeDtypeStruct((nv, cells), F32),
        jax.ShapeDtypeStruct((nv, patches), F32),
    )
    results = pl.pallas_call(
        functools.partial(kernel, n_clump, n_group, cap, half, stride),
        out_shape=tuple(pltpu.VMEM(x.shape, x.dtype) for x in shapes),
        in_specs=[pl.BlockSpec(memory_space=pltpu.SMEM)] + [hbm] * INPUTS,
        out_specs=(vmem, vmem),
        scratch_shapes=[
            buffer, buffer, buffer, buffer, buffer, buffer,
            pltpu.SemaphoreType.DMA((3,)),
            pltpu.SemaphoreType.DMA((3,)),
            pltpu.SemaphoreType.DMA((INPUTS,)),
        ]
        + [
            pltpu.VMEM(x.shape, x.dtype)
            for x in inputs
        ],
        compiler_params=pltpu.CompilerParams(
            collective_id=0, has_side_effects=True, vmem_limit_bytes=48 * 1024 * 1024
        ),
    )(patch_count, *[pltpu.with_memory_space_constraint(x, pltpu.HBM) for x in inputs])
    merged, anomaly = pl.pallas_call(
        store_kernel,
        out_shape=shapes,
        in_specs=[vmem, vmem],
        out_specs=(hbm, hbm),
        scratch_shapes=[pltpu.SemaphoreType.DMA((2,))],
        compiler_params=pltpu.CompilerParams(vmem_limit_bytes=4 * 1024 * 1024),
    )(*results)
    return merged.T, anomaly.T[None]


def solution(mesh):
    split = P(("clump", "grp"))
    return jax.shard_map(
        per_device,
        mesh=mesh,
        in_specs=(split,) * 10 + (P(),) + (split,) * 2,
        out_specs=(split, split),
        check_vma=False,
    )
```
